32 devices in a mesh: mem: 2 (over y), lat: 4 (over z), lon: 4 (over x, core).
Axes of the slice: x: 2, y: 2, z: 4, core: 2. Of those that a mesh axis runs over, the one named last changes fastest.
Arguments:
- control: bfloat16 [62, 3, 4, 4, 73728], P('mem', None, 'lat', 'lon'), may hold values from -6 to 6
- perturbs: bfloat16 [62, 3, 4, 4, 73728], P('mem', None, 'lat', 'lon'), may hold values from -0.75 to 0.75
- static_input: bfloat16 [3, 4, 4, 73728], P(None, 'lat', 'lon'), may hold values from -6 to 6
- lat_basis: bfloat16 [768, 384], replicated, may hold values from -0.21875 to 0.21875
- local_spectrum: float32 [384, 768], P(None, 'lat'), may hold values from 0.1 to 1
- static_spectrum: float32 [384, 768], P(None, 'lat'), may hold values from 0.1 to 1
- static_weight: float32 [3], replicated, may hold values from 0.2 to 0.8
Outputs:
- increment: float32 [3, 4, 4, 73728], P(None, 'lat', 'lon')
The draws below stay inside these ranges and needn't reach their ends.
All inputs are finite; a program needn't handle non-finite values.
Results may differ from the reference program's by a relative error of at most 0.0073.
Values may be sent and summed in bfloat16 or wider, within the bound.
A program may use at most 128 MiB of HBM per device.

```python
import math
import jax
import jax.numpy as jnp
from jax import lax

NLON = 1536
NLAT = 768
KLON = 768
KLAT = 384
LEV = 3
MEMBERS = 62
CELLS = 73728
N_LAT = 4
N_LON = 4


def block_levels(own_key, shape, cuts, low, high):
    factor_of, own = 1.0, jax.random.fold_in(own_key, 6)
    for axis_at, parts in cuts:
        heights = jnp.exp(jax.random.uniform(jax.random.fold_in(own, axis_at), (parts,), jnp.float32, low / len(cuts), high / len(cuts)))
        factor_of = factor_of * jnp.repeat(heights, shape[axis_at] // parts).reshape([-1 if axis == axis_at else 1 for axis in range(len(shape))])
    return factor_of


def gaussian(own_key, dims, scale, limit, shards=(), held_as=jnp.bfloat16):
    result = jax.random.normal(own_key, dims, jnp.float32) * scale
    if len(shards) > 0:
        result = block_levels(own_key, dims, shards, -0.22, 0.18) * result
    return jnp.clip(result, min=-limit, max=limit).astype(held_as)


def setup_inputs(seed: int = 0) -> dict:
    arg_keys = jax.random.split(jax.random.key(seed), 8)
    control = gaussian(arg_keys[0], (MEMBERS, LEV, N_LAT, N_LON, CELLS), 1.0, 6.0, ((0, 2), (2, 4), (3, 4)))
    perturbs = gaussian(arg_keys[1], (MEMBERS, LEV, N_LAT, N_LON, CELLS), 0.125, 0.75, ((0, 2), (2, 4), (3, 4)))
    static_input = gaussian(arg_keys[2], (LEV, N_LAT, N_LON, CELLS), 1.0, 6.0, ((1, 4), (2, 4)))
    lat_basis = gaussian(arg_keys[3], (NLAT, KLAT), NLAT ** -0.5, 0.21875)
    local_spectrum = jnp.clip(jnp.exp(math.log(1.0) - 2.3025851 * jax.random.uniform(arg_keys[4], (KLAT, KLON), jnp.float32) ** block_levels(arg_keys[4], (KLAT, KLON), ((1, 4),), -0.2, 0.2)), 0.1, 1.0)
    static_spectrum = jnp.clip(jnp.exp(math.log(1.0) - 2.3025851 * jax.random.uniform(arg_keys[5], (KLAT, KLON), jnp.float32) ** block_levels(arg_keys[5], (KLAT, KLON), ((1, 4),), -0.2, 0.2)), 0.1, 1.0)
    static_weight = jnp.clip(jax.random.uniform(arg_keys[6], (LEV,), jnp.float32, 0.2, 0.8), 0.2, 0.8)
    return dict(control=control, perturbs=perturbs, static_input=static_input, lat_basis=lat_basis, local_spectrum=local_spectrum, static_spectrum=static_spectrum, static_weight=static_weight)


def zonal_table():
    half = KLON // 2
    points = jnp.arange(NLON, dtype=jnp.int32)
    column = jnp.arange(KLON, dtype=jnp.int32)
    wave = jnp.where(column < half, column, column - half + 1)
    phase = points[:, None] * wave[None, :] % NLON
    angle = 2.0 * jnp.pi / NLON * phase.astype(jnp.float32)
    scale = jnp.sqrt(jnp.float32(2.0 / NLON))
    values = jnp.where(column[None, :] < half, jnp.cos(angle), jnp.sin(angle)) * scale
    return values.astype(jnp.bfloat16)

def to_plain(blocks):
    lead = blocks.shape[:-3]
    count = len(lead)
    lat_rows = NLAT // N_LAT
    lon_cols = NLON // N_LON
    shaped = blocks.reshape(lead + (N_LAT, N_LON, lat_rows, lon_cols))
    shaped = jnp.moveaxis(shaped, count + 2, count + 1)
    return shaped.reshape(lead + (NLAT, NLON))

def to_blocks(plain):
    lead = plain.shape[:-2]
    count = len(lead)
    lat_rows = NLAT // N_LAT
    lon_cols = NLON // N_LON
    shaped = plain.reshape(lead + (N_LAT, lat_rows, N_LON, lon_cols))
    shaped = jnp.moveaxis(shaped, count + 1, count + 2)
    return shaped.reshape(lead + (N_LAT, N_LON, lat_rows * lon_cols))

def filter_fields(fields, spectrum, zonal, merid):
    zonal_f = zonal.astype(jnp.float32)
    merid_f = merid.astype(jnp.float32)
    waves = jnp.einsum('lyn,nk->lyk', fields.astype(jnp.float32), zonal_f).astype(jnp.bfloat16)
    coef = jnp.einsum('lyk,yj->ljk', waves.astype(jnp.float32), merid_f) * spectrum[None]
    scaled = coef.astype(jnp.bfloat16)
    back = jnp.einsum('ljk,yj->lyk', scaled.astype(jnp.float32), merid_f).astype(jnp.bfloat16)
    grid = jnp.einsum('lyk,nk->lyn', back.astype(jnp.float32), zonal_f).astype(jnp.bfloat16)
    return grid

def reference(control, perturbs, static_input, lat_basis, local_spectrum, static_spectrum, static_weight):
    zonal = zonal_table()

    def add_member(total, pair):
        alpha, pert = pair
        grid = filter_fields(to_plain(alpha), local_spectrum, zonal, lat_basis)
        return (total + to_plain(pert).astype(jnp.float32) * grid.astype(jnp.float32), None)
    start = jnp.zeros((LEV, NLAT, NLON), jnp.float32)
    ensemble, unused = lax.scan(add_member, start, (control, perturbs))
    static_part = filter_fields(to_plain(static_input), static_spectrum, zonal, lat_basis).astype(jnp.float32)
    weight = static_weight[:, None, None]
    return to_blocks(weight * static_part + (1.0 - weight) * ensemble)
```

```python
import jax
import jax.numpy as jnp
from jax import lax
from jax.sharding import PartitionSpec as P


NLON = 1536
NLAT = 768
KLON = 768


def zonal_table():
    half = KLON // 2
    points = jnp.arange(NLON, dtype=jnp.int32)
    column = jnp.arange(KLON, dtype=jnp.int32)
    wave = jnp.where(column < half, column, column - half + 1)
    phase = points[:, None] * wave[None, :] % NLON
    angle = 2.0 * jnp.pi / NLON * phase.astype(jnp.float32)
    scale = jnp.sqrt(jnp.float32(2.0 / NLON))
    values = jnp.where(column[None, :] < half, jnp.cos(angle), jnp.sin(angle)) * scale
    return values.astype(jnp.bfloat16)


def swap(block, axis, step):
    if step == 0:
        return block
    pairs = [(i, i ^ step) for i in range(lax.axis_size(axis))]
    return lax.ppermute(block, axis, pairs)


def pick(blocks, index):
    return lax.dynamic_index_in_dim(blocks, index, 0, keepdims=False)


def mul(spec, a, b):
    return jnp.einsum(spec, a, b, preferred_element_type=jnp.float32)


def by_fields(
    control, perturbs, static_input, lat_basis, local_spectrum, static_spectrum, static_weight
):
    mem_dev, levels = control.shape[:2]
    cell_count = control.shape[-1]
    n_lat, n_lon = lax.axis_size("lat"), lax.axis_size("lon")
    rows = NLAT // n_lat
    cols = cell_count // rows
    size = mem_dev + 1
    part = size // n_lon
    own_fields = part // n_lat
    my_lon, my_lat = lax.axis_index("lon"), lax.axis_index("lat")
    strips_basis = zonal_table().reshape(n_lon, cols, KLON)
    near_strips = jnp.stack([pick(strips_basis, my_lon ^ e) for e in range(n_lon)])
    near_zonal = near_strips.reshape(NLON, KLON)
    bands_basis = lat_basis.reshape(n_lat, rows, -1)
    near_bands = jnp.stack([pick(bands_basis, my_lat ^ d) for d in range(n_lat)])
    near_merid = near_bands.reshape(NLAT, -1)
    local_full = lax.all_gather(local_spectrum, "lat", axis=1, tiled=True)
    static_full = lax.all_gather(static_spectrum, "lat", axis=1, tiled=True)
    first = my_lon * part + my_lat * own_fields
    is_static = first + jnp.arange(own_fields, dtype=jnp.int32) == mem_dev
    spectrum = jnp.where(is_static[:, None, None], static_full[None], local_full[None])
    first_mem = (lax.axis_index("mem") == 0).astype(jnp.float32)
    increments = []
    for level in range(levels):
        fields = jnp.concatenate(
            [control[:, level, 0, 0], static_input[level, 0, 0][None]], 0
        ).reshape(n_lon, part, rows, cols)
        strips = [pick(fields, my_lon ^ e) for e in range(n_lon)]
        strips = [swap(strip, "lon", e) for e, strip in enumerate(strips)]
        full_rows = jnp.concatenate(strips, -1)
        waves = mul("fyn,nk->fyk", full_rows, near_zonal).astype(jnp.bfloat16)
        if level == 0:
            waves, perturbs = lax.optimization_barrier((waves, perturbs))
        waves = waves.reshape(n_lat, own_fields, rows, KLON)
        bands = [pick(waves, my_lat ^ d) for d in range(n_lat)]
        bands = [swap(band, "lat", d) for d, band in enumerate(bands)]
        columns = jnp.concatenate(bands, 1)
        coef = mul("fyk,yj->fjk", columns, near_merid)
        scaled = (coef * spectrum).astype(jnp.bfloat16)
        back = [
            mul("fjk,yj->fyk", scaled, near_bands[d]).astype(jnp.bfloat16)
            for d in range(n_lat)
        ]
        back = [swap(block, "lat", d) for d, block in enumerate(back)]
        back = jnp.stack(back)
        rows_back = jnp.concatenate([pick(back, my_lat ^ d) for d in range(n_lat)], 0)
        pert = perturbs[:, level, 0, 0]
        pert = jnp.concatenate([pert, jnp.zeros_like(pert[:1])], 0)
        pert = pert.reshape(n_lon, part, rows, cols)
        ensemble = jnp.zeros((rows, cols), jnp.float32)
        static_part = jnp.zeros((rows, cols), jnp.float32)
        for e in range(n_lon):
            grid = mul("fyk,nk->fyn", rows_back, near_strips[e]).astype(jnp.bfloat16)
            filtered = swap(grid, "lon", e)
            ensemble += mul("fyn,fyn->yn", pick(pert, my_lon ^ e), filtered)
            static_here = (my_lon ^ e) == n_lon - 1
            static_part += jnp.where(static_here, filtered[-1].astype(jnp.float32), 0.0)
        weight = static_weight[level]
        own = first_mem * weight * static_part + (1.0 - weight) * ensemble
        if lax.axis_size("mem") == 2:
            own += swap(own, "mem", 1)
        else:
            own = lax.psum(own, "mem")
        increments.append(own)
    return jnp.stack(increments).reshape(levels, 1, 1, cell_count)


def by_waves(
    control, perturbs, static_input, lat_basis, local_spectrum, static_spectrum, static_weight
):
    mem_dev, levels = (control.shape[0], control.shape[1])
    cell_count = control.shape[-1]
    lat_rows = NLAT // lax.axis_size("lat")
    lon_cols = cell_count // lat_rows
    fields = jnp.concatenate([control, static_input[None]], 0).reshape(-1, lat_rows, lon_cols)
    per_lon = fields.shape[0] // lax.axis_size("lon")
    field_index = lax.axis_index("lon") * per_lon + jnp.arange(per_lon, dtype=jnp.int32)
    is_static = field_index >= mem_dev * levels
    first_mem = (lax.axis_index("mem") == 0).astype(jnp.float32)
    zonal = zonal_table()
    strips = lax.all_to_all(fields, "lon", split_axis=0, concat_axis=2, tiled=True)
    waves = mul("bxn,nk->kbx", strips, zonal).astype(jnp.bfloat16)
    merid = lax.all_to_all(waves, "lat", split_axis=0, concat_axis=2, tiled=True)
    coef = mul("kby,yj->kbj", merid, lat_basis)
    spectrum = jnp.where(
        is_static[None, :, None], static_spectrum.T[:, None, :], local_spectrum.T[:, None, :]
    )
    scaled = (coef * spectrum).astype(jnp.bfloat16)
    back = mul("kbj,yj->kby", scaled, lat_basis).astype(jnp.bfloat16)
    zonal_rows = lax.all_to_all(back, "lat", split_axis=2, concat_axis=0, tiled=True)
    grid = mul("kbx,nk->bxn", zonal_rows, zonal).astype(jnp.bfloat16)
    pert_fields = perturbs.reshape(mem_dev, levels, lat_rows, lon_cols)
    weight = static_weight[:, None, None]
    filtered = lax.all_to_all(grid, "lon", split_axis=2, concat_axis=0, tiled=True).reshape(
        mem_dev + 1, levels, lat_rows, lon_cols
    )
    ensemble = mul("mlxn,mlxn->lxn", pert_fields, filtered[:mem_dev])
    static_part = filtered[mem_dev].astype(jnp.float32)
    own = first_mem * weight * static_part + (1.0 - weight) * ensemble
    total = lax.psum(own, "mem")
    return total.reshape(levels, 1, 1, cell_count)


def solution(mesh):
    def shards(control, *rest):
        group = lax.axis_size("lat") * lax.axis_size("lon")
        uneven = (control.shape[0] + 1) % group or group & (group - 1)
        body = by_waves if uneven else by_fields
        return body(control, *rest)

    return jax.shard_map(
        shards,
        mesh=mesh,
        in_specs=(
            P("mem", None, "lat", "lon", None),
            P("mem", None, "lat", "lon", None),
            P(None, "lat", "lon", None),
            P(),
            P(None, "lat"),
            P(None, "lat"),
            P(),
        ),
        out_specs=P(None, "lat", "lon", None),
        check_vma=False,
    )
```
